8 devices in a mesh: rep: 2 (over y, z), dp: 4 (over x, core).
Axes of the slice: x: 2, y: 2, z: 1, core: 2. Of those that a mesh axis runs over, the one named last changes fastest.
Arguments:
- x: bfloat16 [8, 2048, 1024], P(('rep', 'dp')), parts along dimension 0
- dy: bfloat16 [8, 2048, 1024], P(('rep', 'dp')), parts along dimension 0
- w_gate: bfloat16 [2, 1024, 2816], replicated
- w_up: bfloat16 [2, 1024, 2816], replicated
- w_down: bfloat16 [2, 2816, 1024], replicated
- m_w_gate: float32 [2, 1024, 2816], replicated
- m_w_up: float32 [2, 1024, 2816], replicated
- m_w_down: float32 [2, 2816, 1024], replicated
- v_w_gate: float32 [2, 1024, 2816], replicated
- v_w_up: float32 [2, 1024, 2816], replicated
- v_w_down: float32 [2, 2816, 1024], replicated
Outputs:
- output 1: bfloat16 [4, 1024, 2816], P('rep'), parts along dimension 0
- output 2: bfloat16 [4, 1024, 2816], P('rep'), parts along dimension 0
- output 3: bfloat16 [4, 2816, 1024], P('rep'), parts along dimension 0
- output 4: float32 [4, 1024, 2816], P('rep'), parts along dimension 0
- output 5: float32 [4, 1024, 2816], P('rep'), parts along dimension 0
- output 6: float32 [4, 2816, 1024], P('rep'), parts along dimension 0
- output 7: float32 [4, 1024, 2816], P('rep'), parts along dimension 0
- output 8: float32 [4, 1024, 2816], P('rep'), parts along dimension 0
- output 9: float32 [4, 2816, 1024], P('rep'), parts along dimension 0
There are 2 independent parts. The reference program is written for one: setup_inputs(seed, part) draws one part's arguments, and reference() takes and returns one part's arrays. A program takes and returns all parts, laid end to end along the dimension named above; an argument that names none is the same for every part.
All inputs are finite; a program needn't handle non-finite values.
Results may differ from the reference program's by a relative error of at most 0.022.
Values are sent between devices in bfloat16 or wider.
A program may use at most 2.75 GiB of HBM per device.

```python
import jax
import jax.numpy as jnp
from jax import lax

SEQUENCES = 4
TOKENS = 2048
D = 1024
FF = 2816
LAYERS = 2
NAMES = ("w_gate", "w_up", "w_down")
SHAPES = {"w_gate": (LAYERS, D, FF), "w_up": (LAYERS, D, FF), "w_down": (LAYERS, FF, D)}


def bump(key, n, height):
    away = (jnp.arange(n, dtype=jnp.int32) - jax.random.randint(key, (), 0, n, jnp.int32)) % n
    return jnp.where(away < n // 8, height, 1.0)


def together(key, own, strength):
    shared = jax.random.normal(key, own.shape[1:], jnp.float32)
    return (own + strength * shared) * lax.rsqrt(1 + strength * strength)


def setup_inputs(seed: int = 0, part: int = 0) -> dict:
    kx, kdy, ka, kb, kz, kf, kh, kl, *keys = jax.random.split(jax.random.key(seed), 8 + 3 * len(NAMES))
    kx, kdy, ka, kb = (jax.random.fold_in(k, part) for k in (kx, kdy, ka, kb))
    kw, km, kv = (keys[i::3] for i in range(3))
    shape = (SEQUENCES, TOKENS, D)
    much_x, much_dy = jax.random.uniform(kz, (2,), jnp.float32, 0.0, 1.0)
    loud = 2.0 ** jax.random.uniform(jax.random.fold_in(kz, 1), (), jnp.float32, -1.0, 2.0)
    layers = 2.0 ** jax.random.uniform(kl, (LAYERS, 1, 1), jnp.float32, -1.0, 1.0)
    x = together(ka, jax.random.normal(kx, shape, jnp.float32), much_x) * bump(kf, D, 4.0)
    dy = together(kb, jax.random.normal(kdy, shape, jnp.float32), much_dy)
    drawn = {"x": x.astype(jnp.bfloat16), "dy": (loud * dy * (SEQUENCES * TOKENS) ** -0.5).astype(jnp.bfloat16)}
    for key, name in zip(kw, NAMES, strict=True):
        w = jax.random.normal(key, SHAPES[name], jnp.float32) * SHAPES[name][1] ** -0.5
        drawn[name] = (w * {"w_gate": 1.0, "w_up": bump(kh, FF, 4.0), "w_down": layers}[name]).astype(jnp.bfloat16)
    for key, name in zip(km, NAMES, strict=True):
        drawn[f"m_{name}"] = 0.1 * jax.random.normal(key, SHAPES[name], jnp.float32)
    for key, name in zip(kv, NAMES, strict=True):
        drawn[f"v_{name}"] = jax.random.uniform(key, SHAPES[name], jnp.float32, 0.005, 0.015)
    return drawn


def matmul(a, w):
    return jnp.dot(a, w, preferred_element_type=jnp.float32).astype(jnp.bfloat16)


def normed(h):
    wide = h.astype(jnp.float32)
    scale = lax.rsqrt(jnp.mean(wide**2, -1, keepdims=True) + 1e-6)
    return (wide * scale).astype(jnp.bfloat16)


def layer(h, w):
    a = normed(h)
    gate = jnp.dot(a, w["w_gate"], preferred_element_type=jnp.float32)
    up = jnp.dot(a, w["w_up"], preferred_element_type=jnp.float32)
    return h + matmul((jax.nn.silu(gate) * up).astype(jnp.bfloat16), w["w_down"])


def adamw(w, m, v, g):
    m = 0.9 * m + 0.1 * g
    v = 0.95 * v + 0.05 * g * g
    step = m * lax.rsqrt(v + 1e-8) + 0.1 * w
    return (w - 0.02 * step).astype(jnp.bfloat16), m, v


def clipped(gradients, sum_of_squares, count):
    factor = jnp.minimum(1.0, 0.5 * lax.rsqrt(sum_of_squares / count + 1e-30))
    return [g * factor for g in gradients]


def stack(weights, h):
    return lax.scan(lambda h, w: (layer(h, w), None), h, weights)[0]


def reference(x, dy, w_gate, w_up, w_down, m_w_gate, m_w_up, m_w_down, v_w_gate, v_w_up, v_w_down):
    weights = dict(zip(NAMES, (w_gate, w_up, w_down), strict=True))

    def take(so_far, sequence):
        h, by_y = sequence
        _, back = jax.vjp(lambda w: stack(w, h), weights)
        return jax.tree.map(lambda total, term: total + term.astype(jnp.float32), so_far, back(by_y)[0]), None

    none_yet = {name: jnp.zeros(w.shape, jnp.float32) for name, w in weights.items()}
    by_weights, _ = lax.scan(take, none_yet, (x, dy))
    gradients = [by_weights[name].astype(jnp.bfloat16).astype(jnp.float32) for name in NAMES]
    gradients = clipped(gradients, sum(jnp.sum(g * g) for g in gradients), sum(g.size for g in gradients))
    new = [
        adamw(w.astype(jnp.float32), m, v, g)
        for w, m, v, g in zip((w_gate, w_up, w_down), (m_w_gate, m_w_up, m_w_down), (v_w_gate, v_w_up, v_w_down), gradients, strict=True)
    ]
    return tuple(one[which] for which in range(3) for one in new)
```

```python
import functools

import jax
import jax.numpy as jnp
import numpy as np
from jax import lax
from jax.experimental import pallas as pl
from jax.experimental.pallas import tpu as pltpu
from jax.sharding import PartitionSpec as P

BF, F32 = jnp.bfloat16, jnp.float32
T, D, FF = 2048, 1024, 2816
FT = 256
NT = FF // FT
HALF, QUARTER = D // 2, D // 4
CHUNK = 512
NC = T // CHUNK
X_SWAP = [(0, 2), (2, 0), (1, 3), (3, 1)]
CORE_SWAP = [(0, 1), (1, 0), (2, 3), (3, 2)]
VMEM_LIMIT = 64 * 1000 * 1000
EPS = 1e-6


def dot(a, b):
    return jnp.dot(a, b, preferred_element_type=F32)


def dot_nt(a, b):
    return lax.dot_general(a, b, (((1,), (1,)), ((), ())), preferred_element_type=F32)


def params(n=1):
    return pltpu.CompilerParams(dimension_semantics=("arbitrary",) * n, vmem_limit_bytes=VMEM_LIMIT)


def cost(matmuls, nbytes):
    return pl.CostEstimate(flops=int(matmuls * 2 * T * D * FF), bytes_accessed=int(nbytes), transcendentals=0)


def norm(h):
    wide = h.astype(F32)
    return wide * lax.rsqrt(jnp.mean(wide * wide, -1, keepdims=True) + EPS)


def whole(shape):
    return pl.BlockSpec(shape, lambda *_: (0,) * len(shape))


def gate_up_kernel(h_ref, wg_ref, wu_ref, act_ref, gate_ref, up_ref, at_ref, a_ref):
    @pl.when(pl.program_id(0) == 0)
    def _():
        for r in range(NC):
            rows = slice(r * CHUNK, (r + 1) * CHUNK)
            a = norm(h_ref[rows, :]).astype(BF)
            a_ref[rows, :] = a
            at_ref[:, rows] = a.T

    for r in range(NC):
        rows = slice(r * CHUNK, (r + 1) * CHUNK)
        gate = dot(a_ref[rows, :], wg_ref[...])
        up = dot(a_ref[rows, :], wu_ref[...])
        gate_ref[rows, :] = gate
        up_ref[rows, :] = up
        act_ref[rows, :] = (gate * jax.nn.sigmoid(gate) * up).astype(BF)


def gate_up(h, wg, wu, layer):
    weight = pl.BlockSpec((None, D, FT), lambda j: (layer, 0, j))
    tile = pl.BlockSpec((T, FT), lambda j: (0, j))
    return pl.pallas_call(
        gate_up_kernel,
        grid=(NT,),
        in_specs=[whole((T, D)), weight, weight],
        out_specs=[tile, tile, tile, whole((D, T))],
        out_shape=[
            jax.ShapeDtypeStruct((T, FF), BF),
            jax.ShapeDtypeStruct((T, FF), F32),
            jax.ShapeDtypeStruct((T, FF), F32),
            jax.ShapeDtypeStruct((D, T), BF),
        ],
        scratch_shapes=[pltpu.VMEM((T, D), BF)],
        compiler_params=params(),
        cost_estimate=cost(2, 75e6),
        name="gate_up",
    )(h, wg, wu)


def down_kernel(act_ref, w_ref, h_ref, out_ref, a_ref, at_ref):
    h = h_ref[...] + dot(act_ref[...], w_ref[...]).astype(BF)
    out_ref[...] = h
    a = norm(h).astype(BF)
    a_ref[...] = a
    at_ref[...] = a.T


def down(act, w, h, layer):
    rows = pl.BlockSpec((CHUNK, D), lambda i: (i, 0))
    return pl.pallas_call(
        down_kernel,
        grid=(NC,),
        in_specs=[
            pl.BlockSpec((CHUNK, FF), lambda i: (i, 0)),
            pl.BlockSpec((None, FF, D), lambda i: (layer, 0, 0)),
            rows,
        ],
        out_specs=[rows, rows, pl.BlockSpec((D, CHUNK), lambda i: (0, i))],
        out_shape=[
            jax.ShapeDtypeStruct((T, D), BF),
            jax.ShapeDtypeStruct((T, D), BF),
            jax.ShapeDtypeStruct((D, T), BF),
        ],
        compiler_params=params(),
        cost_estimate=cost(1, 30e6),
        name="down",
    )(act, w, h)


def turn_kernel(x_ref, xt_ref):
    xt_ref[...] = x_ref[...].T


def norm_turn_kernel(h_ref, x_ref, a_ref, at_ref, xt_ref):
    a = norm(h_ref[...]).astype(BF)
    a_ref[...] = a
    at_ref[...] = a.T
    xt_ref[...] = x_ref[...].T


def turn(x):
    return pl.pallas_call(
        turn_kernel,
        grid=(NC,),
        in_specs=[pl.BlockSpec((CHUNK, D), lambda i: (i, 0))],
        out_specs=pl.BlockSpec((D, CHUNK), lambda i: (0, i)),
        out_shape=jax.ShapeDtypeStruct((D, T), BF),
        compiler_params=params(),
        cost_estimate=cost(0.2, 8e6),
        name="turn",
    )(x)


def norm_turn(h, x):
    rows = pl.BlockSpec((CHUNK, D), lambda i: (i, 0))
    columns = pl.BlockSpec((D, CHUNK), lambda i: (0, i))
    return pl.pallas_call(
        norm_turn_kernel,
        grid=(NC,),
        in_specs=[rows, rows],
        out_specs=[rows, columns, columns],
        out_shape=[jax.ShapeDtypeStruct((T, D), BF), jax.ShapeDtypeStruct((D, T), BF), jax.ShapeDtypeStruct((D, T), BF)],
        compiler_params=params(),
        cost_estimate=cost(0.4, 20e6),
        name="norm_turn",
    )(h, x)


def gated(gate, up, by_act):
    by_act = by_act.astype(BF).astype(F32)
    sig = jax.nn.sigmoid(gate)
    silu = gate * sig
    by_gate = by_act * up * (sig + silu * (1.0 - sig))
    return (silu * up).astype(BF), by_gate.astype(BF), (by_act * silu).astype(BF)


def hidden_kernel(a_ref, by_ref, wg_ref, wu_ref, wd_ref, act_ref, dg_ref, du_ref):
    for r in range(NC):
        rows = slice(r * CHUNK, (r + 1) * CHUNK)
        gate = dot(a_ref[rows, :], wg_ref[...])
        up = dot(a_ref[rows, :], wu_ref[...])
        by_act = dot_nt(by_ref[rows, :], wd_ref[...])
        act_ref[rows, :], dg_ref[rows, :], du_ref[rows, :] = gated(gate, up, by_act)


def hidden(a, by, wg, wu, wd, layer):
    weight = pl.BlockSpec((None, D, FT), lambda j: (layer, 0, j))
    tile = pl.BlockSpec((T, FT), lambda j: (0, j))
    return pl.pallas_call(
        hidden_kernel,
        grid=(NT,),
        in_specs=[whole((T, D)), whole((T, D)), weight, weight, pl.BlockSpec((None, FT, D), lambda j: (layer, j, 0))],
        out_specs=[tile, tile, tile],
        out_shape=[jax.ShapeDtypeStruct((T, FF), BF)] * 3,
        compiler_params=params(),
        cost_estimate=cost(3, 60e6),
        name="hidden",
    )(a, by, wg, wu, wd)


def states_kernel(dg_ref, du_ref, wg_ref, wu_ref, h_ref, by_ref, out_ref, outt_ref):
    by_a = dot_nt(dg_ref[...], wg_ref[...]).astype(BF) + dot_nt(du_ref[...], wu_ref[...]).astype(BF)
    wide = h_ref[...].astype(F32)
    by_a = by_a.astype(F32)
    scale = lax.rsqrt(jnp.mean(wide * wide, -1, keepdims=True) + EPS)
    inner = jnp.mean(by_a * wide, -1, keepdims=True)
    by_h = by_a * scale - wide * (inner * scale * scale * scale)
    out = by_ref[...] + by_h.astype(BF)
    out_ref[...] = out
    outt_ref[...] = out.T


def states(dg, du, wg, wu, h, by, layer):
    tm = 256
    rows = pl.BlockSpec((tm, D), lambda i: (i, 0))
    hidden_rows = pl.BlockSpec((tm, FF), lambda i: (i, 0))
    weight = pl.BlockSpec((None, D, FF), lambda i: (layer, 0, 0))
    return pl.pallas_call(
        states_kernel,
        grid=(T // tm,),
        in_specs=[hidden_rows, hidden_rows, weight, weight, rows, rows],
        out_specs=[rows, pl.BlockSpec((D, tm), lambda i: (0, i))],
        out_shape=[jax.ShapeDtypeStruct((T, D), BF), jax.ShapeDtypeStruct((D, T), BF)],
        compiler_params=params(),
        cost_estimate=cost(2, 45e6),
        name="states",
    )(dg, du, wg, wu, h, by)


def halves(core_ref):
    keep = pl.ds(pl.multiple_of(core_ref[0] * HALF, HALF), HALF)
    send = pl.ds(pl.multiple_of((1 - core_ref[0]) * HALF, HALF), HALF)
    return keep, send


def first_weights_kernel(core_ref, at_ref, byt_ref, by_ref, gate_ref, up_ref, wd_ref, keep_ref, send_ref, act_ref, dg_ref, du_ref):
    for r in range(NC):
        rows = slice(r * CHUNK, (r + 1) * CHUNK)
        by_act = dot_nt(by_ref[rows, :], wd_ref[...])
        act_ref[rows, :], dg_ref[rows, :], du_ref[rows, :] = gated(gate_ref[rows, :], up_ref[rows, :], by_act)
    keep, send = halves(core_ref)
    for half, out_ref in ((send, send_ref), (keep, keep_ref)):
        out_ref[0] = dot(at_ref[half, :], dg_ref[...]).astype(BF)
        out_ref[1] = dot(at_ref[half, :], du_ref[...]).astype(BF)
        out_ref[2] = dot(byt_ref[half, :], act_ref[...]).astype(BF)


def first_weights(core, at, byt, by, gate, up, wd, layer, start, tiles):
    tile = pl.BlockSpec((T, FT), lambda j, _: (0, start + j))
    out = pl.BlockSpec((3, HALF, FT), lambda j, _: (0, 0, j))
    return pl.pallas_call(
        first_weights_kernel,
        grid_spec=pltpu.PrefetchScalarGridSpec(
            num_scalar_prefetch=1,
            grid=(tiles,),
            in_specs=[
                whole((D, T)),
                whole((D, T)),
                whole((T, D)),
                tile,
                tile,
                pl.BlockSpec((None, FT, D), lambda j, _: (layer, start + j, 0)),
            ],
            out_specs=[out, out],
            scratch_shapes=[pltpu.VMEM((T, FT), BF)] * 3,
        ),
        out_shape=[jax.ShapeDtypeStruct((3, HALF, tiles * FT), BF)] * 2,
        compiler_params=params(),
        cost_estimate=cost(4 * tiles / NT, 80e6 * tiles / NT),
        name="first_weights",
    )(core, at, byt, by, gate, up, wd)


def last_weights_kernel(
    core_ref, at_ref, byt_ref, a2_ref, by2_ref, at2_ref, byt2_ref, act_ref, dg_ref, du_ref, wg_ref, wu_ref, wd_ref,
    keep_ref, send_ref, act2_ref, dg2_ref, du2_ref,
):
    for r in range(NC):
        rows = slice(r * CHUNK, (r + 1) * CHUNK)
        gate = dot(a2_ref[rows, :], wg_ref[...])
        up = dot(a2_ref[rows, :], wu_ref[...])
        by_act = dot_nt(by2_ref[rows, :], wd_ref[...])
        act2_ref[rows, :], dg2_ref[rows, :], du2_ref[rows, :] = gated(gate, up, by_act)
    keep, send = halves(core_ref)
    for half, out_ref in ((send, send_ref), (keep, keep_ref)):
        out_ref[0] = (dot(at_ref[half, :], dg_ref[...]) + dot(at2_ref[half, :], dg2_ref[...])).astype(BF)
        out_ref[1] = (dot(at_ref[half, :], du_ref[...]) + dot(at2_ref[half, :], du2_ref[...])).astype(BF)
        out_ref[2] = (dot(byt_ref[half, :], act_ref[...]) + dot(byt2_ref[half, :], act2_ref[...])).astype(BF)


def last_weights(core, at, byt, a2, by2, at2, byt2, act, dg, du, wg, wu, wd, layer, start, tiles):
    tile = pl.BlockSpec((T, FT), lambda j, _: (0, start + j))
    weight = pl.BlockSpec((None, D, FT), lambda j, _: (layer, 0, start + j))
    out = pl.BlockSpec((3, HALF, FT), lambda j, _: (0, 0, j))
    return pl.pallas_call(
        last_weights_kernel,
        grid_spec=pltpu.PrefetchScalarGridSpec(
            num_scalar_prefetch=1,
            grid=(tiles,),
            in_specs=[
                whole((D, T)), whole((D, T)), whole((T, D)), whole((T, D)), whole((D, T)), whole((D, T)),
                tile, tile, tile, weight, weight,
                pl.BlockSpec((None, FT, D), lambda j, _: (layer, start + j, 0)),
            ],
            out_specs=[out, out],
            scratch_shapes=[pltpu.VMEM((T, FT), BF)] * 3,
        ),
        out_shape=[jax.ShapeDtypeStruct((3, HALF, tiles * FT), BF)] * 2,
        compiler_params=params(),
        cost_estimate=cost(9 * tiles / NT, 90e6 * tiles / NT),
        name="last_weights",
    )(core, at, byt, a2, by2, at2, byt2, act, dg, du, wg, wu, wd)


def adamw(w, m, v, g):
    m = 0.9 * m + 0.1 * g
    v = 0.95 * v + 0.05 * g * g
    step = m * lax.rsqrt(v + 1e-8) + 0.1 * w
    return (w - 0.02 * step).astype(BF), m, v


def adamw_kernel(ranges, n_alias, table_ref, factor_ref, *refs):
    n = len(ranges)
    gradients, refs = refs[:n], refs[n:]
    ins, outs = refs[:9], refs[9 + n_alias :]
    step = pl.program_id(0)
    for g_ref, (first, last) in zip(gradients, ranges, strict=True):

        @pl.when((step >= first) & (step < last))
        def _(g_ref=g_ref):
            factor = factor_ref[0]
            for i in range(3):
                g = g_ref[i].astype(F32) * factor
                if i == 2:
                    g = g.T
                new = adamw(ins[i][...].astype(F32), ins[3 + i][...], ins[6 + i][...], g)
                for which in range(3):
                    outs[3 * which + i][...] = new[which]


def adamw_steps(segments):
    steps = []
    for g, layer, row, start in segments:
        steps += [(layer, row + r, start + f) for r in range(g.shape[1] // ROWS) for f in range(g.shape[2] // FT)]
    return steps


def adamw_blocks(segments, table, begin, factor, arrays, so_far):
    ranges, steps = [], 0
    for g, *_ in segments:
        more = (g.shape[1] // ROWS) * (g.shape[2] // FT)
        ranges.append((steps, steps + more))
        steps += more

    def g_spec(g, start, stop):
        broad = g.shape[2] // FT

        def index(s, *_):
            own = jnp.clip(s - start, 0, stop - start - 1)
            return 0, own // broad, own % broad

        return pl.BlockSpec((3, ROWS, FT), index)

    wide = pl.BlockSpec((None, ROWS, FT), lambda s, t, _: (t[0, s + begin], t[1, s + begin], t[2, s + begin]))
    tall = pl.BlockSpec((None, FT, ROWS), lambda s, t, _: (t[0, s + begin], t[2, s + begin], t[1, s + begin]))
    nine = [wide, wide, tall] * 3
    gradients = [s[0] for s in segments]
    n = len(gradients)
    alias = {2 + n + 9 + i: i for i in range(9)} if so_far else {}
    shapes = [jax.ShapeDtypeStruct(a.shape, BF if i < 3 else F32) for i, a in enumerate(arrays)]
    return pl.pallas_call(
        functools.partial(adamw_kernel, ranges, len(so_far)),
        grid_spec=pltpu.PrefetchScalarGridSpec(
            num_scalar_prefetch=2,
            grid=(steps,),
            in_specs=[g_spec(g, *r) for g, r in zip(gradients, ranges, strict=True)] + nine + [pl.BlockSpec(memory_space=pl.ANY)] * len(so_far),
            out_specs=nine,
        ),
        out_shape=shapes,
        input_output_aliases=alias,
        compiler_params=params(),
        cost_estimate=cost(2.5 * steps / (4 * NT), 190e6 * steps / (4 * NT)),
        name="adamw",
    )(table, factor, *gradients, *arrays, *so_far)


ROWS = QUARTER
FIRST_PARTS = ((0, 6), (6, 5))
LAST_PARTS = ((0, 3), (3, 4), (7, 4))


def solution(mesh):
    def step(x, dy, *arrays):
        wg, wu, wd = arrays[:3]
        me = lax.axis_index("dp")
        chip, core = me >> 1, me & 1
        core_ref = core.astype(jnp.int32).reshape(1)

        def swap_x(a):
            return lax.ppermute(a, "dp", X_SWAP)

        def swap_core(a):
            return lax.ppermute(a, "dp", CORE_SWAP)

        h0, by2 = x[0], dy[0]
        by2_other = swap_x(by2)
        act0, gate0, up0, a0t = gate_up(h0, wg, wu, 0)
        h1, a1, a1t = down(act0, wd, h0, 0)
        h1_other = swap_x(h1)
        act1, dg1, du1 = hidden(a1, by2, wg, wu, wd, 1)
        by1, by1t = states(dg1, du1, wg, wu, h1, by2, 1)
        by2t = turn(by2)

        def piece(g, row):
            return lax.dynamic_slice_in_dim(g, row, QUARTER, 1).astype(F32)

        first = []
        for start, tiles in FIRST_PARTS:
            keep, send = first_weights(core_ref, a0t, by1t, by1, gate0, up0, wd, 0, start, tiles)
            first.append((keep, swap_core(send)))
        partial = []
        for keep, got in first:
            away = (1 - chip) * QUARTER
            away = (piece(keep, away) + piece(got, away)).astype(BF)
            partial.append(swap_x(away))

        a1o, a1ot, by2ot = norm_turn(h1_other, by2_other)
        last = []
        for start, tiles in LAST_PARTS:
            keep, send = last_weights(
                core_ref, a1t, by2t, a1o, by2_other, a1ot, by2ot, act1, dg1, du1, wg, wu, wd, 1, start, tiles,
            )
            last.append((keep, swap_core(send)))

        squares0, squares1 = jnp.zeros((), F32), jnp.zeros((), F32)
        quarters, halves_ = [], []
        for (keep, got), far in zip(first, partial, strict=True):
            mine = (piece(keep, chip * QUARTER) + piece(got, chip * QUARTER) + far.astype(F32)).astype(BF)
            squares0 += jnp.sum(jnp.square(mine.astype(F32)))
            quarters.append(mine)
        for keep, got in last:
            mine = (keep.astype(F32) + got.astype(F32)).astype(BF)
            squares1 += jnp.sum(jnp.square(mine.astype(F32)))
            halves_.append(mine)

        squares0 = squares0.reshape(1, 1)
        squares0 = squares0 + swap_x(squares0)
        squares = squares0 + squares1.reshape(1, 1)
        squares = (squares + swap_core(squares)).reshape(1)
        count = sum(a.size for a in arrays[:3])
        factor = jnp.minimum(1.0, 0.5 * lax.rsqrt(squares / count + 1e-30))

        core_halves = [swap_core(h) for h in halves_]
        far_quarters = [swap_x(q) for q in quarters]
        core_quarters = [swap_core(q) for q in quarters]
        core_far_quarters = [swap_core(q) for q in far_quarters]

        def segments(layer, row, parts, gradients):
            return [(g, layer, row, part[0]) for g, part in zip(gradients, parts, strict=True)]

        groups = [
            segments(1, 0, LAST_PARTS, halves_),
            segments(1, 2, LAST_PARTS, core_halves),
            segments(0, 0, FIRST_PARTS, quarters) + segments(0, 2, FIRST_PARTS, core_quarters),
            segments(0, 1, FIRST_PARTS, far_quarters) + segments(0, 3, FIRST_PARTS, core_far_quarters),
        ]
        steps = [adamw_steps(group) for group in groups]
        table = np.array(sum(steps, []), np.int32).T
        owns = jnp.where(table[0] == 0, 2 * core + chip, 2 * core).astype(jnp.int32)
        table = jnp.asarray(table) ^ (jnp.asarray([[0], [1], [0]], jnp.int32) * owns)
        out, begin = [], 0
        for n, group in enumerate(groups):
            out = adamw_blocks(group, table, begin, factor, arrays, out)
            begin += len(steps[n])
        return tuple(out)

    return jax.shard_map(
        step,
        mesh=mesh,
        in_specs=(P(("rep", "dp"), None, None),) * 2 + (P(None, None, None),) * 9,
        out_specs=(P("rep", None, None),) * 9,
        check_vma=False,
    )
```

```python
import functools

import jax
import jax.numpy as jnp
import numpy as np
from jax import lax
from jax.experimental import pallas as pl
from jax.experimental.pallas import tpu as pltpu
from jax.sharding import PartitionSpec as P

BF, F32 = jnp.bfloat16, jnp.float32
T, D, FF = 2048, 1024, 2816
FT = 256
NT = FF // FT
HALF, QUARTER = D // 2, D // 4
CHUNK = 512
NC = T // CHUNK
ROWS, BROAD, SOME, UNROLL = QUARTER, FF // 2, 16, 2
TURN = 256
X_SWAP = [(0, 2), (2, 0), (1, 3), (3, 1)]
CORE_SWAP = [(0, 1), (1, 0), (2, 3), (3, 2)]
VMEM_LIMIT = 64 * 1000 * 1000
EPS = 1e-6


def dot(a, b):
    return jnp.dot(a, b, preferred_element_type=F32)


def dot_nt(a, b):
    return lax.dot_general(a, b, (((1,), (1,)), ((), ())), preferred_element_type=F32)


def params(**more):
    if more:
        more["has_side_effects"] = True
    return pltpu.CompilerParams(dimension_semantics=("arbitrary",), vmem_limit_bytes=VMEM_LIMIT, **more)


def cost(matmuls, nbytes):
    return pl.CostEstimate(flops=int(matmuls * 2 * T * D * FF), bytes_accessed=int(nbytes), transcendentals=0)


def norm(h):
    wide = h.astype(F32)
    return wide * lax.rsqrt(jnp.mean(wide * wide, -1, keepdims=True) + EPS)


def whole(shape):
    return pl.BlockSpec(shape, lambda *_: (0,) * len(shape))


def gate_up_kernel(h_ref, wg_ref, wu_ref, act_ref, gate_ref, up_ref, at_ref, a_ref):
    @pl.when(pl.program_id(0) == 0)
    def _():
        for r in range(NC):
            rows = slice(r * CHUNK, (r + 1) * CHUNK)
            a = norm(h_ref[rows, :]).astype(BF)
            a_ref[rows, :] = a
            at_ref[:, rows] = a.T

    for r in range(NC):
        rows = slice(r * CHUNK, (r + 1) * CHUNK)
        gate = dot(a_ref[rows, :], wg_ref[...])
        up = dot(a_ref[rows, :], wu_ref[...])
        gate_ref[rows, :] = gate
        up_ref[rows, :] = up
        act_ref[rows, :] = (gate * jax.nn.sigmoid(gate) * up).astype(BF)


def gate_up(h, wg, wu, layer):
    weight = pl.BlockSpec((None, D, FT), lambda j: (layer, 0, j))
    tile = pl.BlockSpec((T, FT), lambda j: (0, j))
    return pl.pallas_call(
        gate_up_kernel,
        grid=(NT,),
        in_specs=[whole((T, D)), weight, weight],
        out_specs=[tile, tile, tile, whole((D, T))],
        out_shape=[
            jax.ShapeDtypeStruct((T, FF), BF),
            jax.ShapeDtypeStruct((T, FF), F32),
            jax.ShapeDtypeStruct((T, FF), F32),
            jax.ShapeDtypeStruct((D, T), BF),
        ],
        scratch_shapes=[pltpu.VMEM((T, D), BF)],
        compiler_params=params(),
        cost_estimate=cost(2, 75e6),
        name="gate_up",
    )(h, wg, wu)


def down_kernel(act_ref, w_ref, h_ref, out_ref, a_ref, at_ref):
    h = h_ref[...] + dot(act_ref[...], w_ref[...]).astype(BF)
    out_ref[...] = h
    a = norm(h).astype(BF)
    a_ref[...] = a
    at_ref[...] = a.T


def down(act, w, h, layer):
    rows = pl.BlockSpec((CHUNK, D), lambda i: (i, 0))
    return pl.pallas_call(
        down_kernel,
        grid=(NC,),
        in_specs=[
            pl.BlockSpec((CHUNK, FF), lambda i: (i, 0)),
            pl.BlockSpec((None, FF, D), lambda i: (layer, 0, 0)),
            rows,
        ],
        out_specs=[rows, rows, pl.BlockSpec((D, CHUNK), lambda i: (0, i))],
        out_shape=[
            jax.ShapeDtypeStruct((T, D), BF),
            jax.ShapeDtypeStruct((T, D), BF),
            jax.ShapeDtypeStruct((D, T), BF),
        ],
        compiler_params=params(),
        cost_estimate=cost(1, 30e6),
        name="down",
    )(act, w, h)


def norm_turn_kernel(h_ref, x_ref, a_ref, at_ref, xt_ref):
    a = norm(h_ref[...]).astype(BF)
    a_ref[...] = a
    at_ref[...] = a.T
    xt_ref[...] = x_ref[...].T


def norm_turn(h, x):
    rows = pl.BlockSpec((CHUNK, D), lambda i: (i, 0))
    columns = pl.BlockSpec((D, CHUNK), lambda i: (0, i))
    return pl.pallas_call(
        norm_turn_kernel,
        grid=(NC,),
        in_specs=[rows, rows],
        out_specs=[rows, columns, columns],
        out_shape=[jax.ShapeDtypeStruct((T, D), BF), jax.ShapeDtypeStruct((D, T), BF), jax.ShapeDtypeStruct((D, T), BF)],
        compiler_params=params(),
        cost_estimate=cost(0.4, 20e6),
        name="norm_turn",
    )(h, x)


def gated(gate, up, by_act):
    by_act = by_act.astype(BF).astype(F32)
    sig = jax.nn.sigmoid(gate)
    silu = gate * sig
    by_gate = by_act * up * (sig + silu * (1.0 - sig))
    return (silu * up).astype(BF), by_gate.astype(BF), (by_act * silu).astype(BF)


def hidden_kernel(a_ref, by_ref, wg_ref, wu_ref, wd_ref, act_ref, dg_ref, du_ref, byt_ref):
    turned = jnp.minimum(pl.program_id(0), T // TURN - 1)
    byt_ref[...] = by_ref[pl.ds(pl.multiple_of(turned * TURN, TURN), TURN), :].T
    for r in range(NC):
        rows = slice(r * CHUNK, (r + 1) * CHUNK)
        gate = dot(a_ref[rows, :], wg_ref[...])
        up = dot(a_ref[rows, :], wu_ref[...])
        by_act = dot_nt(by_ref[rows, :], wd_ref[...])
        act_ref[rows, :], dg_ref[rows, :], du_ref[rows, :] = gated(gate, up, by_act)


def hidden(a, by, wg, wu, wd, layer):
    weight = pl.BlockSpec((None, D, FT), lambda j: (layer, 0, j))
    tile = pl.BlockSpec((T, FT), lambda j: (0, j))
    return pl.pallas_call(
        hidden_kernel,
        grid=(NT,),
        in_specs=[whole((T, D)), whole((T, D)), weight, weight, pl.BlockSpec((None, FT, D), lambda j: (layer, j, 0))],
        out_specs=[tile, tile, tile, pl.BlockSpec((D, TURN), lambda j: (0, jnp.minimum(j, T // TURN - 1)))],
        out_shape=[jax.ShapeDtypeStruct((T, FF), BF)] * 3 + [jax.ShapeDtypeStruct((D, T), BF)],
        compiler_params=params(),
        cost_estimate=cost(3, 60e6),
        name="hidden",
    )(a, by, wg, wu, wd)


def states_kernel(dg_ref, du_ref, wg_ref, wu_ref, h_ref, by_ref, out_ref, outt_ref):
    by_a = dot_nt(dg_ref[...], wg_ref[...]).astype(BF) + dot_nt(du_ref[...], wu_ref[...]).astype(BF)
    wide = h_ref[...].astype(F32)
    by_a = by_a.astype(F32)
    scale = lax.rsqrt(jnp.mean(wide * wide, -1, keepdims=True) + EPS)
    inner = jnp.mean(by_a * wide, -1, keepdims=True)
    by_h = by_a * scale - wide * (inner * scale * scale * scale)
    out = by_ref[...] + by_h.astype(BF)
    out_ref[...] = out
    outt_ref[...] = out.T


def states(dg, du, wg, wu, h, by, layer):
    tm = 256
    rows = pl.BlockSpec((tm, D), lambda i: (i, 0))
    hidden_rows = pl.BlockSpec((tm, FF), lambda i: (i, 0))
    weight = pl.BlockSpec((None, D, FF), lambda i: (layer, 0, 0))
    return pl.pallas_call(
        states_kernel,
        grid=(T // tm,),
        in_specs=[hidden_rows, hidden_rows, weight, weight, rows, rows],
        out_specs=[rows, pl.BlockSpec((D, tm), lambda i: (0, i))],
        out_shape=[jax.ShapeDtypeStruct((T, D), BF), jax.ShapeDtypeStruct((D, T), BF)],
        compiler_params=params(),
        cost_estimate=cost(2, 45e6),
        name="states",
    )(dg, du, wg, wu, h, by)


def positions():
    me = lax.axis_index("dp")
    return lax.div(me, 2), lax.rem(me, 2), me + 1 - 2 * lax.rem(me, 2)


def part(index, size):
    return pl.ds(pl.multiple_of(index * size, size), size)


class Exchange:
    scratch = (
        pltpu.VMEM((2, 3, HALF, FT), BF),
        pltpu.VMEM((3, 3, HALF, FT), F32),
        pltpu.VMEM((NT, 3, HALF, FT), BF),
        pltpu.SemaphoreType.DMA((NT,)),
        pltpu.SemaphoreType.DMA((NT,)),
    )

    def __init__(self, sent, kept, got, send_sem, got_sem):
        self.sent, self.kept, self.got = sent, kept, got
        self.send_sem, self.got_sem = send_sem, got_sem
        self.chip, self.core, self.other = positions()

    def greet(self):
        barrier = pltpu.get_barrier_semaphore()
        pl.semaphore_signal(barrier, inc=1, device_id={"dp": self.other}, device_id_type=pl.DeviceIdType.MESH)
        pl.semaphore_wait(barrier, 1)

    def copy(self, j):
        return pltpu.make_async_remote_copy(
            src_ref=self.sent.at[lax.rem(j, 2)],
            dst_ref=self.got.at[j],
            send_sem=self.send_sem.at[j],
            recv_sem=self.got_sem.at[j],
            device_id={"dp": self.other},
            device_id_type=pl.DeviceIdType.MESH,
        )

    def put(self, j, products):
        for i, g in enumerate(products(part(1 - self.core, HALF))):
            self.sent[lax.rem(j, 2), i] = g.astype(BF)
        for i, g in enumerate(products(part(self.core, HALF))):
            self.kept[lax.rem(j, 3), i] = g

    def total(self, j, i, rows):
        return self.kept[lax.rem(j, 3), i, rows, :] + self.got[j, i, rows, :].astype(F32)


def exchange_steps(exchange, loads, early, compute, finish):
    j = pl.program_id(0)

    @pl.when(j == 0)
    def _():
        for load in loads:
            load.start()
        exchange.greet()
        for load in loads[:early]:
            load.wait()

    @pl.when(j >= 2)
    def _():
        exchange.copy(j - 2).wait()

    def late():
        @pl.when(j == 0)
        def _():
            for load in loads[early:]:
                load.wait()

    @pl.when(j < 2)
    def _():
        compute(j, late)

    @pl.when((j >= 2) & (j < NT))
    def _():
        finish(j - 2)
        compute(j, None)

    @pl.when(j < NT)
    def _():
        exchange.copy(j).start()

    @pl.when(j >= NT)
    def _():
        finish(j - 2)


def first_weights_kernel(
    at_any, byt_any, by_any, gate_ref, up_ref, wd_ref, home_ref, away_ref,
    at_ref, byt_ref, by_ref, act_ref, dg_ref, du_ref, load_sem, *exchange,
):
    exchange = Exchange(*exchange)
    pairs = ((by_any, by_ref), (at_any, at_ref), (byt_any, byt_ref))
    loads = [pltpu.make_async_copy(a, b, load_sem.at[n]) for n, (a, b) in enumerate(pairs)]

    def compute(j, late):
        for r in range(NC):
            rows = slice(r * CHUNK, (r + 1) * CHUNK)
            by_act = dot_nt(by_ref[rows, :], wd_ref[...])
            act_ref[rows, :], dg_ref[rows, :], du_ref[rows, :] = gated(gate_ref[rows, :], up_ref[rows, :], by_act)
        if late:
            late()
        exchange.put(
            j,
            lambda half: (dot(a[half, :], b[...]) for a, b in ((at_ref, dg_ref), (at_ref, du_ref), (byt_ref, act_ref))),
        )

    def finish(j):
        for i in range(3):
            home_ref[i] = exchange.total(j, i, part(exchange.chip, QUARTER))
            away_ref[i] = exchange.total(j, i, part(1 - exchange.chip, QUARTER)).astype(BF)

    exchange_steps(exchange, loads, 1, compute, finish)


def tile_now(j):
    return jnp.minimum(j, NT - 1)


def tile_done(j):
    return jnp.clip(j - 2, 0, NT - 1)


ANY = pl.BlockSpec(memory_space=pl.ANY)


def first_weights(at, byt, by, gate, up, wd, layer):
    tile = pl.BlockSpec((T, FT), lambda j: (0, tile_now(j)))
    out = pl.BlockSpec((3, QUARTER, FT), lambda j: (0, 0, tile_done(j)))
    return pl.pallas_call(
        first_weights_kernel,
        grid=(NT + 2,),
        in_specs=[ANY, ANY, ANY, tile, tile, pl.BlockSpec((None, FT, D), lambda j: (layer, tile_now(j), 0))],
        out_specs=[out, out],
        out_shape=[jax.ShapeDtypeStruct((3, QUARTER, FF), F32), jax.ShapeDtypeStruct((3, QUARTER, FF), BF)],
        scratch_shapes=[
            pltpu.VMEM((D, T), BF),
            pltpu.VMEM((D, T), BF),
            pltpu.VMEM((T, D), BF),
            *[pltpu.VMEM((T, FT), BF)] * 3,
            pltpu.SemaphoreType.DMA((3,)),
            *Exchange.scratch,
        ],
        compiler_params=params(collective_id=0),
        cost_estimate=cost(4, 80e6),
        name="first_weights",
    )(at, byt, by, gate, up, wd)


def last_weights_kernel(
    at_any, byt_any, a2_any, by2_any, at2_any, byt2_any, act_ref, dg_ref, du_ref, wg_ref, wu_ref, wd_ref, mine_ref, squares_ref,
    at_ref, byt_ref, a2_ref, by2_ref, at2_ref, byt2_ref, act2_ref, dg2_ref, du2_ref, load_sem, *exchange,
):
    exchange = Exchange(*exchange)
    pairs = (
        (a2_any, a2_ref), (by2_any, by2_ref), (at_any, at_ref), (at2_any, at2_ref), (byt_any, byt_ref), (byt2_any, byt2_ref),
    )
    loads = [pltpu.make_async_copy(a, b, load_sem.at[n]) for n, (a, b) in enumerate(pairs)]

    @pl.when(pl.program_id(0) == 0)
    def _():
        squares_ref[...] = jnp.zeros_like(squares_ref)

    def compute(j, late):
        for r in range(NC):
            rows = slice(r * CHUNK, (r + 1) * CHUNK)
            gate = dot(a2_ref[rows, :], wg_ref[...])
            up = dot(a2_ref[rows, :], wu_ref[...])
            by_act = dot_nt(by2_ref[rows, :], wd_ref[...])
            act2_ref[rows, :], dg2_ref[rows, :], du2_ref[rows, :] = gated(gate, up, by_act)
        if late:
            late()
        fours = ((at_ref, dg_ref, at2_ref, dg2_ref), (at_ref, du_ref, at2_ref, du2_ref), (byt_ref, act_ref, byt2_ref, act2_ref))
        exchange.put(j, lambda half: (dot(a[half, :], b[...]) + dot(c[half, :], d[...]) for a, b, c, d in fours))

    def finish(j):
        squares = squares_ref[...]
        for i in range(3):
            for r in range(4):
                rows = slice(r * HALF // 4, (r + 1) * HALF // 4)
                mine = exchange.total(j, i, rows).astype(BF)
                mine_ref[i, rows, :] = mine
                wide = mine.astype(F32)
                squares += jnp.sum((wide * wide).reshape(-1, 8, FT), 0)
        squares_ref[...] = squares

    exchange_steps(exchange, loads, 2, compute, finish)


def last_weights(at, byt, a2, by2, at2, byt2, act, dg, du, wg, wu, wd, layer):
    tile = pl.BlockSpec((T, FT), lambda j: (0, tile_now(j)))
    weight = pl.BlockSpec((None, D, FT), lambda j: (layer, 0, tile_now(j)))
    return pl.pallas_call(
        last_weights_kernel,
        grid=(NT + 2,),
        in_specs=[ANY] * 6
        + [tile, tile, tile, weight, weight, pl.BlockSpec((None, FT, D), lambda j: (layer, tile_now(j), 0))],
        out_specs=[pl.BlockSpec((3, HALF, FT), lambda j: (0, 0, tile_done(j))), pl.BlockSpec((8, FT), lambda j: (0, 0))],
        out_shape=[jax.ShapeDtypeStruct((3, HALF, FF), BF), jax.ShapeDtypeStruct((8, FT), F32)],
        scratch_shapes=[
            pltpu.VMEM((D, T), BF), pltpu.VMEM((D, T), BF), pltpu.VMEM((T, D), BF),
            pltpu.VMEM((T, D), BF), pltpu.VMEM((D, T), BF), pltpu.VMEM((D, T), BF),
            *[pltpu.VMEM((T, FT), BF)] * 3,
            pltpu.SemaphoreType.DMA((6,)),
            *Exchange.scratch,
        ],
        compiler_params=params(collective_id=1),
        cost_estimate=cost(9, 90e6),
        name="last_weights",
    )(at, byt, a2, by2, at2, byt2, act, dg, du, wg, wu, wd)


def adamw(w, m, v, g):
    m = 0.9 * m + 0.1 * g
    v = 0.95 * v + 0.05 * g * g
    step = m * lax.rsqrt(v + 1e-8) + 0.1 * w
    return (w - 0.02 * step).astype(BF), m, v


def adamw_kernel(ranges, n_alias, table_ref, factor_ref, *refs):
    n = len(ranges)
    gradients, refs = refs[:n], refs[n:]
    ins, outs, turned_ref = refs[:9], refs[9 + n_alias : 18 + n_alias], refs[-1]
    step = pl.program_id(0)
    for g_ref, (first, last) in zip(gradients, ranges, strict=True):

        @pl.when((step >= first) & (step < last))
        def _(g_ref=g_ref):
            factor = factor_ref[0]
            turned_ref[...] = g_ref[2].T
            for i in range(3):

                def some(r, _, i=i):
                    rows = pl.ds(pl.multiple_of(r * SOME, SOME), SOME)
                    g = (turned_ref[rows, :] if i == 2 else g_ref[i, rows, :]).astype(F32) * factor
                    new = adamw(ins[i][rows, :].astype(F32), ins[3 + i][rows, :], ins[6 + i][rows, :], g)
                    for which in range(3):
                        outs[3 * which + i][rows, :] = new[which]
                    return _

                lax.fori_loop(0, (BROAD if i == 2 else ROWS) // SOME, some, 0, unroll=UNROLL)


def adamw_steps(segments):
    steps = []
    for g, layer, row, start in segments:
        steps += [(layer, row + r, start + f) for r in range(g.shape[1] // ROWS) for f in range(g.shape[2] // BROAD)]
    return steps


def adamw_blocks(segments, table, begin, factor, arrays, so_far):
    ranges, steps = [], 0
    for g, *_ in segments:
        more = (g.shape[1] // ROWS) * (g.shape[2] // BROAD)
        ranges.append((steps, steps + more))
        steps += more

    def g_spec(g, start, stop):
        broad = g.shape[2] // BROAD

        def index(s, *_):
            own = jnp.clip(s - start, 0, stop - start - 1)
            return 0, own // broad, own % broad

        return pl.BlockSpec((3, ROWS, BROAD), index)

    wide = pl.BlockSpec((None, ROWS, BROAD), lambda s, t, _: (t[0, s + begin], t[1, s + begin], t[2, s + begin]))
    tall = pl.BlockSpec((None, BROAD, ROWS), lambda s, t, _: (t[0, s + begin], t[2, s + begin], t[1, s + begin]))
    nine = [wide, wide, tall] * 3
    gradients = [s[0] for s in segments]
    n = len(gradients)
    alias = {2 + n + 9 + i: i for i in range(9)} if so_far else {}
    shapes = [jax.ShapeDtypeStruct(a.shape, BF if i < 3 else F32) for i, a in enumerate(arrays)]
    return pl.pallas_call(
        functools.partial(adamw_kernel, ranges, len(so_far)),
        grid_spec=pltpu.PrefetchScalarGridSpec(
            num_scalar_prefetch=2,
            grid=(steps,),
            in_specs=[g_spec(g, *r) for g, r in zip(gradients, ranges, strict=True)] + nine + [pl.BlockSpec(memory_space=pl.ANY)] * len(so_far),
            out_specs=nine,
            scratch_shapes=[pltpu.VMEM((BROAD, ROWS), BF)],
        ),
        out_shape=shapes,
        input_output_aliases=alias,
        compiler_params=params(),
        cost_estimate=cost(2.5 * steps / (4 * 4), 190e6 * steps / (4 * 4)),
        name="adamw",
    )(table, factor, *gradients, *arrays, *so_far)


def solution(mesh):
    def step(x, dy, *arrays):
        wg, wu, wd = arrays[:3]
        me = lax.axis_index("dp")
        chip, core = me >> 1, me & 1

        def swap_x(a):
            return lax.ppermute(a, "dp", X_SWAP)

        def swap_core(a):
            return lax.ppermute(a, "dp", CORE_SWAP)

        h0, by2 = x[0], dy[0]
        by2_other = swap_x(by2)
        act0, gate0, up0, a0t = gate_up(h0, wg, wu, 0)
        h1, a1, a1t = down(act0, wd, h0, 0)
        h1_other = swap_x(h1)
        act1, dg1, du1, by2t = hidden(a1, by2, wg, wu, wd, 1)
        by1, by1t = states(dg1, du1, wg, wu, h1, by2, 1)
        home, away = first_weights(a0t, by1t, by1, gate0, up0, wd, 0)
        far = swap_x(away)
        a1o, a1ot, by2ot = norm_turn(h1_other, by2_other)
        half, squares1 = last_weights(a1t, by2t, a1o, by2_other, a1ot, by2ot, act1, dg1, du1, wg, wu, wd, 1)
        core_half = swap_core(half)
        quarter = (home + far.astype(F32)).astype(BF)
        squares0 = jnp.sum(jnp.square(quarter.astype(F32)))

        squares0 = squares0.reshape(1, 1)
        squares0 = squares0 + swap_x(squares0)
        squares = squares0 + jnp.sum(squares1).reshape(1, 1)
        squares = (squares + swap_core(squares)).reshape(1)
        count = sum(a.size for a in arrays[:3])
        factor = jnp.minimum(1.0, 0.5 * lax.rsqrt(squares / count + 1e-30))

        far_quarter = swap_x(quarter)
        core_quarter = swap_core(quarter)
        core_far = swap_core(far_quarter)

        groups = [
            [(half, 1, 0, 0), (quarter, 0, 0, 0), (core_half, 1, 2, 0), (core_quarter, 0, 2, 0)],
            [(far_quarter, 0, 1, 0), (core_far, 0, 3, 0)],
        ]
        steps = [adamw_steps(group) for group in groups]
        table = np.array(sum(steps, []), np.int32).T
        owns = jnp.where(table[0] == 0, 2 * core + chip, 2 * core).astype(jnp.int32)
        table = jnp.asarray(table) ^ (jnp.asarray([[0], [1], [0]], jnp.int32) * owns)
        out, begin = [], 0
        for n, group in enumerate(groups):
            out = adamw_blocks(group, table, begin, factor, arrays, out)
            begin += len(steps[n])
        return tuple(out)

    return jax.shard_map(
        step,
        mesh=mesh,
        in_specs=(P(("rep", "dp"), None, None),) * 2 + (P(None, None, None),) * 9,
        out_specs=(P("rep", None, None),) * 9,
        check_vma=False,
    )
```

```python
import functools

import jax
import jax.numpy as jnp
import numpy as np
from jax import lax
from jax.experimental import pallas as pl
from jax.experimental.pallas import tpu as pltpu
from jax.sharding import PartitionSpec as P

BF, F32 = jnp.bfloat16, jnp.float32
T, D, FF = 2048, 1024, 2816
FT = 256
NT = FF // FT
HALF, QUARTER = D // 2, D // 4
CHUNK = 512
NC = T // CHUNK
ROWS, BROAD, SOME, UNROLL = QUARTER, FF // 2, 16, 2
TURN = 256
X_SWAP = [(0, 2), (2, 0), (1, 3), (3, 1)]
CORE_SWAP = [(0, 1), (1, 0), (2, 3), (3, 2)]
VMEM_LIMIT = 64 * 1000 * 1000
EPS = 1e-6


def dot(a, b):
    return jnp.dot(a, b, preferred_element_type=F32)


def dot_nt(a, b):
    return lax.dot_general(a, b, (((1,), (1,)), ((), ())), preferred_element_type=F32)


def params(**more):
    if more:
        more["has_side_effects"] = True
    return pltpu.CompilerParams(dimension_semantics=("arbitrary",), vmem_limit_bytes=VMEM_LIMIT, **more)


def cost(matmuls, nbytes):
    return pl.CostEstimate(flops=int(matmuls * 2 * T * D * FF), bytes_accessed=int(nbytes), transcendentals=0)


def norm(h):
    wide = h.astype(F32)
    return wide * lax.rsqrt(jnp.mean(wide * wide, -1, keepdims=True) + EPS)


def part(index, size):
    return pl.ds(pl.multiple_of(index * size, size), size)


def tile_now(j):
    return jnp.minimum(j, NT - 1)


def whole(shape):
    return pl.BlockSpec(shape, lambda *_: (0,) * len(shape))


def forward_kernel(
    h_ref, wg_ref, wu_ref, wd_ref, act_ref, silu_ref, slope_ref, at_ref, out_ref, a1_ref, a1t_ref, a_ref, total_ref
):
    j = pl.program_id(0)

    @pl.when(j == 0)
    def _():
        def some(r, _):
            rows = part(r, TURN)
            a = norm(h_ref[rows, :]).astype(BF)
            a_ref[rows, :] = a
            at_ref[:, rows] = a.T
            total_ref[rows, :] = jnp.zeros((TURN, D), F32)
            return _

        lax.fori_loop(0, T // TURN, some, 0)

    @pl.when(j < NT)
    def _():
        for r in range(NC):
            rows = slice(r * CHUNK, (r + 1) * CHUNK)
            gate = dot(a_ref[rows, :], wg_ref[...])
            up = dot(a_ref[rows, :], wu_ref[...])
            sig = jax.nn.sigmoid(gate)
            silu = gate * sig
            act_ref[rows, :] = (silu * up).astype(BF)
            silu_ref[rows, :] = silu
            slope_ref[rows, :] = up * (sig + silu * (1.0 - sig))
            total_ref[rows, :] += dot(act_ref[rows, :], wd_ref[...])

    @pl.when(j >= NT)
    def _():
        rows = part(j - NT, CHUNK)
        h = h_ref[rows, :] + total_ref[rows, :].astype(BF)
        out_ref[...] = h
        a = norm(h).astype(BF)
        a1_ref[...] = a
        a1t_ref[...] = a.T


def forward(h, wg, wu, wd, layer):
    weight = pl.BlockSpec((None, D, FT), lambda j: (layer, 0, tile_now(j)))
    tile = pl.BlockSpec((None, T, FT), lambda j: (tile_now(j), 0, 0))
    rows = pl.BlockSpec((CHUNK, D), lambda j: (jnp.maximum(j - NT, 0), 0))
    return pl.pallas_call(
        forward_kernel,
        grid=(NT + NC,),
        in_specs=[whole((T, D)), weight, weight, pl.BlockSpec((None, FT, D), lambda j: (layer, tile_now(j), 0))],
        out_specs=[tile, tile, tile, whole((D, T)), rows, rows, pl.BlockSpec((D, CHUNK), lambda j: (0, jnp.maximum(j - NT, 0)))],
        out_shape=[
            jax.ShapeDtypeStruct((NT, T, FT), BF),
            jax.ShapeDtypeStruct((NT, T, FT), F32),
            jax.ShapeDtypeStruct((NT, T, FT), F32),
            jax.ShapeDtypeStruct((D, T), BF),
            jax.ShapeDtypeStruct((T, D), BF),
            jax.ShapeDtypeStruct((T, D), BF),
            jax.ShapeDtypeStruct((D, T), BF),
        ],
        scratch_shapes=[pltpu.VMEM((T, D), BF), pltpu.VMEM((T, D), F32)],
        compiler_params=params(),
        cost_estimate=cost(3, 90e6),
        name="forward",
    )(h, wg, wu, wd)


def gated(gate, up, by_act):
    by_act = by_act.astype(BF).astype(F32)
    sig = jax.nn.sigmoid(gate)
    silu = gate * sig
    by_gate = by_act * up * (sig + silu * (1.0 - sig))
    return (silu * up).astype(BF), by_gate.astype(BF), (by_act * silu).astype(BF)


def hidden_kernel(a_ref, by_ref, wg_ref, wu_ref, wd_ref, act_ref, dg_ref, du_ref, byt_ref):
    turned = jnp.minimum(pl.program_id(0), T // TURN - 1)
    byt_ref[...] = by_ref[pl.ds(pl.multiple_of(turned * TURN, TURN), TURN), :].T
    for r in range(NC):
        rows = slice(r * CHUNK, (r + 1) * CHUNK)
        gate = dot(a_ref[rows, :], wg_ref[...])
        up = dot(a_ref[rows, :], wu_ref[...])
        by_act = dot_nt(by_ref[rows, :], wd_ref[...])
        act_ref[rows, :], dg_ref[rows, :], du_ref[rows, :] = gated(gate, up, by_act)


def hidden(a, by, wg, wu, wd, layer):
    weight = pl.BlockSpec((None, D, FT), lambda j: (layer, 0, j))
    tile = pl.BlockSpec((T, FT), lambda j: (0, j))
    return pl.pallas_call(
        hidden_kernel,
        grid=(NT,),
        in_specs=[whole((T, D)), whole((T, D)), weight, weight, pl.BlockSpec((None, FT, D), lambda j: (layer, j, 0))],
        out_specs=[tile, tile, tile, pl.BlockSpec((D, TURN), lambda j: (0, jnp.minimum(j, T // TURN - 1)))],
        out_shape=[jax.ShapeDtypeStruct((T, FF), BF)] * 3 + [jax.ShapeDtypeStruct((D, T), BF)],
        compiler_params=params(),
        cost_estimate=cost(3, 60e6),
        name="hidden",
    )(a, by, wg, wu, wd)


def states_kernel(dg_ref, du_ref, wg_ref, wu_ref, h_ref, by_ref, out_ref, outt_ref):
    by_a = dot_nt(dg_ref[...], wg_ref[...]).astype(BF) + dot_nt(du_ref[...], wu_ref[...]).astype(BF)
    wide = h_ref[...].astype(F32)
    by_a = by_a.astype(F32)
    scale = lax.rsqrt(jnp.mean(wide * wide, -1, keepdims=True) + EPS)
    inner = jnp.mean(by_a * wide, -1, keepdims=True)
    by_h = by_a * scale - wide * (inner * scale * scale * scale)
    out = by_ref[...] + by_h.astype(BF)
    out_ref[...] = out
    outt_ref[...] = out.T


def states(dg, du, wg, wu, h, by, layer):
    tm = 256
    rows = pl.BlockSpec((tm, D), lambda i: (i, 0))
    hidden_rows = pl.BlockSpec((tm, FF), lambda i: (i, 0))
    weight = pl.BlockSpec((None, D, FF), lambda i: (layer, 0, 0))
    return pl.pallas_call(
        states_kernel,
        grid=(T // tm,),
        in_specs=[hidden_rows, hidden_rows, weight, weight, rows, rows],
        out_specs=[rows, pl.BlockSpec((D, tm), lambda i: (0, i))],
        out_shape=[jax.ShapeDtypeStruct((T, D), BF), jax.ShapeDtypeStruct((D, T), BF)],
        compiler_params=params(),
        cost_estimate=cost(2, 45e6),
        name="states",
    )(dg, du, wg, wu, h, by)


def positions():
    me = lax.axis_index("dp")
    return lax.div(me, 2), lax.rem(me, 2), me + 1 - 2 * lax.rem(me, 2)


ORDER_OF_THREE = (2, 0, 1)


class Exchange:
    scratch = (
        pltpu.VMEM((2, 3, HALF, FT), BF),
        pltpu.VMEM((3, 3, HALF, FT), F32),
        pltpu.VMEM((NT, 3, HALF, FT), BF),
        pltpu.SemaphoreType.DMA((NT,)),
        pltpu.SemaphoreType.DMA((NT,)),
    )

    def __init__(self, sent, kept, got, send_sem, got_sem):
        self.sent, self.kept, self.got = sent, kept, got
        self.send_sem, self.got_sem = send_sem, got_sem
        self.chip, self.core, self.other = positions()

    def greet(self):
        barrier = pltpu.get_barrier_semaphore()
        pl.semaphore_signal(barrier, inc=1, device_id={"dp": self.other}, device_id_type=pl.DeviceIdType.MESH)
        pl.semaphore_wait(barrier, 1)

    def copy(self, j):
        return pltpu.make_async_remote_copy(
            src_ref=self.sent.at[lax.rem(j, 2)],
            dst_ref=self.got.at[j],
            send_sem=self.send_sem.at[j],
            recv_sem=self.got_sem.at[j],
            device_id={"dp": self.other},
            device_id_type=pl.DeviceIdType.MESH,
        )

    def put(self, j, products):
        for i, g in zip(ORDER_OF_THREE, products(part(1 - self.core, HALF))):
            self.sent[lax.rem(j, 2), i] = g.astype(BF)
        for i, g in zip(ORDER_OF_THREE, products(part(self.core, HALF))):
            self.kept[lax.rem(j, 3), i] = g

    def total(self, j, i, rows):
        return self.kept[lax.rem(j, 3), i, rows, :] + self.got[j, i, rows, :].astype(F32)


def exchange_steps(exchange, loads, early, prepare, compute, finish):
    j = pl.program_id(0)

    @pl.when(j == 0)
    def _():
        for load in loads:
            load.start()
        exchange.greet()
        for load in loads[:early]:
            load.wait()
        if prepare:
            prepare()
        for load in loads[early:]:
            load.wait()

    @pl.when(j >= 2)
    def _():
        exchange.copy(j - 2).wait()
        finish(j - 2)

    @pl.when(j < NT)
    def _():
        compute(j)
        exchange.copy(j).start()


def first_weights_kernel(
    at_any, byt_any, by_any, act_ref, silu_ref, slope_ref, wd_ref, home_ref, away_ref, at_ref, byt_ref, by_ref, dg_ref, du_ref,
    load_sem, *exchange,
):
    exchange = Exchange(*exchange)
    pairs = ((by_any, by_ref), (at_any, at_ref), (byt_any, byt_ref))
    loads = [pltpu.make_async_copy(a, b, load_sem.at[n]) for n, (a, b) in enumerate(pairs)]

    def compute(j):
        for r in range(NC):
            rows = slice(r * CHUNK, (r + 1) * CHUNK)
            by_act = dot_nt(by_ref[rows, :], wd_ref[...]).astype(BF).astype(F32)
            dg_ref[rows, :] = (by_act * slope_ref[rows, :]).astype(BF)
            du_ref[rows, :] = (by_act * silu_ref[rows, :]).astype(BF)
        exchange.put(
            j,
            lambda half: (dot(a[half, :], b[...]) for a, b in ((byt_ref, act_ref), (at_ref, dg_ref), (at_ref, du_ref))),
        )

    def finish(j):
        for i in range(3):
            home_ref[i] = exchange.total(j, i, part(exchange.chip, QUARTER))
            away_ref[i] = exchange.total(j, i, part(1 - exchange.chip, QUARTER)).astype(BF)

    exchange_steps(exchange, loads, 1, None, compute, finish)


def tile_done(j):
    return jnp.clip(j - 2, 0, NT - 1)


ANY = pl.BlockSpec(memory_space=pl.ANY)


def first_weights(at, byt, by, act, silu, slope, wd, layer):
    tile = pl.BlockSpec((None, T, FT), lambda j: (tile_now(j), 0, 0))
    out = pl.BlockSpec((3, QUARTER, FT), lambda j: (0, 0, tile_done(j)))
    return pl.pallas_call(
        first_weights_kernel,
        grid=(NT + 2,),
        in_specs=[ANY, ANY, ANY, tile, tile, tile, pl.BlockSpec((None, FT, D), lambda j: (layer, tile_now(j), 0))],
        out_specs=[out, out],
        out_shape=[jax.ShapeDtypeStruct((3, QUARTER, FF), F32), jax.ShapeDtypeStruct((3, QUARTER, FF), BF)],
        scratch_shapes=[
            pltpu.VMEM((D, T), BF),
            pltpu.VMEM((D, T), BF),
            pltpu.VMEM((T, D), BF),
            *[pltpu.VMEM((T, FT), BF)] * 2,
            pltpu.SemaphoreType.DMA((3,)),
            *Exchange.scratch,
        ],
        compiler_params=params(collective_id=0),
        cost_estimate=cost(4, 80e6),
        name="first_weights",
    )(at, byt, by, act, silu, slope, wd)


def last_weights_kernel(
    at_any, byt_any, h2_any, by2_any, act_ref, dg_ref, du_ref, wg_ref, wu_ref, wd_ref, mine_ref, squares_ref,
    at_ref, byt_ref, a2_ref, by2_ref, at2_ref, byt2_ref, act2_ref, dg2_ref, du2_ref, load_sem, *exchange,
):
    exchange = Exchange(*exchange)
    pairs = ((h2_any, a2_ref), (by2_any, by2_ref), (at_any, at_ref), (byt_any, byt_ref))
    loads = [pltpu.make_async_copy(a, b, load_sem.at[n]) for n, (a, b) in enumerate(pairs)]

    def prepare():
        squares_ref[...] = jnp.zeros_like(squares_ref)

        def some(r, _):
            rows = part(r, TURN)
            byt2_ref[:, rows] = by2_ref[rows, :].T
            a = norm(a2_ref[rows, :]).astype(BF)
            a2_ref[rows, :] = a
            at2_ref[:, rows] = a.T
            return _

        lax.fori_loop(0, T // TURN, some, 0)

    def compute(j):
        for r in range(NC):
            rows = slice(r * CHUNK, (r + 1) * CHUNK)
            gate = dot(a2_ref[rows, :], wg_ref[...])
            up = dot(a2_ref[rows, :], wu_ref[...])
            by_act = dot_nt(by2_ref[rows, :], wd_ref[...])
            act2_ref[rows, :], dg2_ref[rows, :], du2_ref[rows, :] = gated(gate, up, by_act)
        fours = ((byt_ref, act_ref, byt2_ref, act2_ref), (at_ref, dg_ref, at2_ref, dg2_ref), (at_ref, du_ref, at2_ref, du2_ref))
        exchange.put(j, lambda half: (dot(a[half, :], b[...]) + dot(c[half, :], d[...]) for a, b, c, d in fours))

    def finish(j):
        squares = squares_ref[...]
        for i in range(3):
            for r in range(4):
                rows = slice(r * HALF // 4, (r + 1) * HALF // 4)
                mine = exchange.total(j, i, rows).astype(BF)
                mine_ref[i, rows, :] = mine
                wide = mine.astype(F32)
                squares += jnp.sum((wide * wide).reshape(-1, 8, FT), 0)
        squares_ref[...] = squares

    exchange_steps(exchange, loads, 2, prepare, compute, finish)


def last_weights(at, byt, h2, by2, act, dg, du, wg, wu, wd, layer):
    tile = pl.BlockSpec((T, FT), lambda j: (0, tile_now(j)))
    weight = pl.BlockSpec((None, D, FT), lambda j: (layer, 0, tile_now(j)))
    return pl.pallas_call(
        last_weights_kernel,
        grid=(NT + 2,),
        in_specs=[ANY] * 4
        + [tile, tile, tile, weight, weight, pl.BlockSpec((None, FT, D), lambda j: (layer, tile_now(j), 0))],
        out_specs=[pl.BlockSpec((3, HALF, FT), lambda j: (0, 0, tile_done(j))), pl.BlockSpec((8, FT), lambda j: (0, 0))],
        out_shape=[jax.ShapeDtypeStruct((3, HALF, FF), BF), jax.ShapeDtypeStruct((8, FT), F32)],
        scratch_shapes=[
            pltpu.VMEM((D, T), BF), pltpu.VMEM((D, T), BF), pltpu.VMEM((T, D), BF),
            pltpu.VMEM((T, D), BF), pltpu.VMEM((D, T), BF), pltpu.VMEM((D, T), BF),
            *[pltpu.VMEM((T, FT), BF)] * 3,
            pltpu.SemaphoreType.DMA((4,)),
            *Exchange.scratch,
        ],
        compiler_params=params(collective_id=1),
        cost_estimate=cost(9, 90e6),
        name="last_weights",
    )(at, byt, h2, by2, act, dg, du, wg, wu, wd)


def home_kernel(home_ref, far_ref, squares1_ref, left_ref, right_ref, squares_ref, total_ref):
    j = pl.program_id(0)

    @pl.when(j == 0)
    def _():
        total_ref[...] = jnp.zeros_like(total_ref)

    for half, out_ref in enumerate((left_ref, right_ref)):
        columns = slice(half * BROAD, (half + 1) * BROAD)

        def some(r, total, columns=columns, out_ref=out_ref):
            rows = part(r, 16)
            mine = (home_ref[rows, columns] + far_ref[rows, columns].astype(F32)).astype(BF)
            out_ref[rows, :] = mine
            wide = mine.astype(F32)
            wide = wide * wide
            return total + wide[:8] + wide[8:]

        total_ref[...] = lax.fori_loop(0, QUARTER // 32, some, total_ref[...], unroll=2)

    @pl.when(j == pl.num_programs(0) - 1)
    def _():
        squares_ref[0, 0] = jnp.sum(total_ref[...])
        squares_ref[0, 1] = jnp.sum(squares1_ref[...])


def home_sum(home, far, squares1):
    block = pl.BlockSpec((None, QUARTER // 2, FF), lambda s: (s // 2, s % 2, 0))
    out = pl.BlockSpec((None, QUARTER // 2, BROAD), lambda s: (s // 2, s % 2, 0))
    return pl.pallas_call(
        home_kernel,
        grid=(6,),
        in_specs=[block, block, whole((8, FT))],
        out_specs=[out, out, pl.BlockSpec(memory_space=pltpu.SMEM)],
        out_shape=[jax.ShapeDtypeStruct((3, QUARTER, BROAD), BF)] * 2 + [jax.ShapeDtypeStruct((1, 2), F32)],
        scratch_shapes=[pltpu.VMEM((8, BROAD), F32)],
        compiler_params=params(),
        cost_estimate=cost(0.2, 18e6),
        name="home_sum",
    )(home, far, squares1)


def adamw(w, m, v, g):
    m = 0.9 * m + 0.1 * g
    v = 0.95 * v + 0.05 * g * g
    step = m * lax.rsqrt(v + 1e-8) + 0.1 * w
    return (w - 0.02 * step).astype(BF), m, v


def adamw_kernel(ranges, n_alias, table_ref, factor_ref, *refs):
    n = len(ranges)
    gradients, refs = refs[:n], refs[n:]
    ins, outs, turned_ref = refs[:9], refs[9 + n_alias : 18 + n_alias], refs[-1]
    step = pl.program_id(0)
    for g_ref, (first, last) in zip(gradients, ranges, strict=True):

        @pl.when((step >= first) & (step < last))
        def _(g_ref=g_ref):
            factor = factor_ref[0]
            turned_ref[...] = g_ref[2].T
            for i in range(3):

                def some(r, _, i=i):
                    rows = pl.ds(pl.multiple_of(r * SOME, SOME), SOME)
                    g = (turned_ref[rows, :] if i == 2 else g_ref[i, rows, :]).astype(F32) * factor
                    new = adamw(ins[i][rows, :].astype(F32), ins[3 + i][rows, :], ins[6 + i][rows, :], g)
                    for which in range(3):
                        outs[3 * which + i][rows, :] = new[which]
                    return _

                lax.fori_loop(0, (BROAD if i == 2 else ROWS) // SOME, some, 0, unroll=UNROLL)


def adamw_steps(segments):
    steps = []
    for g, layer, row, start in segments:
        steps += [(layer, row + r, start + f) for r in range(g.shape[1] // ROWS) for f in range(g.shape[2] // BROAD)]
    return steps


def adamw_blocks(segments, table, begin, factor, arrays, so_far):
    ranges, steps = [], 0
    for g, *_ in segments:
        more = (g.shape[1] // ROWS) * (g.shape[2] // BROAD)
        ranges.append((steps, steps + more))
        steps += more

    def g_spec(g, start, stop):
        broad = g.shape[2] // BROAD

        def index(s, *_):
            own = jnp.clip(s - start, 0, stop - start - 1)
            return 0, own // broad, own % broad

        return pl.BlockSpec((3, ROWS, BROAD), index)

    wide = pl.BlockSpec((None, ROWS, BROAD), lambda s, t, _: (t[0, s + begin], t[1, s + begin], t[2, s + begin]))
    tall = pl.BlockSpec((None, BROAD, ROWS), lambda s, t, _: (t[0, s + begin], t[2, s + begin], t[1, s + begin]))
    nine = [wide, wide, tall] * 3
    gradients = [s[0] for s in segments]
    n = len(gradients)
    alias = {2 + n + 9 + i: i for i in range(9)} if so_far else {}
    shapes = [jax.ShapeDtypeStruct(a.shape, BF if i < 3 else F32) for i, a in enumerate(arrays)]
    return pl.pallas_call(
        functools.partial(adamw_kernel, ranges, len(so_far)),
        grid_spec=pltpu.PrefetchScalarGridSpec(
            num_scalar_prefetch=2,
            grid=(steps,),
            in_specs=[g_spec(g, *r) for g, r in zip(gradients, ranges, strict=True)] + nine + [pl.BlockSpec(memory_space=pl.ANY)] * len(so_far),
            out_specs=nine,
            scratch_shapes=[pltpu.VMEM((BROAD, ROWS), BF)],
        ),
        out_shape=shapes,
        input_output_aliases=alias,
        compiler_params=params(),
        cost_estimate=cost(2.5 * steps / (4 * 4), 190e6 * steps / (4 * 4)),
        name="adamw",
    )(table, factor, *gradients, *arrays, *so_far)


def solution(mesh):
    def step(x, dy, *arrays):
        wg, wu, wd = arrays[:3]
        me = lax.axis_index("dp")
        chip, core = me >> 1, me & 1

        def swap_x(a):
            return lax.ppermute(a, "dp", X_SWAP)

        def swap_core(a):
            return lax.ppermute(a, "dp", CORE_SWAP)

        h0, by2 = x[0], dy[0]
        by2_other = swap_x(by2)
        act0, silu0, slope0, a0t, h1, a1, a1t = forward(h0, wg, wu, wd, 0)
        h1_other = swap_x(h1)
        act1, dg1, du1, by2t = hidden(a1, by2, wg, wu, wd, 1)
        by1, by1t = states(dg1, du1, wg, wu, h1, by2, 1)
        home, away = first_weights(a0t, by1t, by1, act0, silu0, slope0, wd, 0)
        far = swap_x(away)
        half, squares1 = last_weights(a1t, by2t, h1_other, by2_other, act1, dg1, du1, wg, wu, wd, 1)
        core_half = swap_core(half)
        *quarter, squares = home_sum(home, far, squares1)

        squares0, squares1 = squares[:, :1], squares[:, 1:]
        squares = squares0 + swap_x(squares0) + squares1
        squares = (squares + swap_core(squares)).reshape(1)
        count = sum(a.size for a in arrays[:3])
        factor = jnp.minimum(1.0, 0.5 * lax.rsqrt(squares / count + 1e-30))

        far_quarter = [swap_x(q) for q in quarter]
        core_quarter = [swap_core(q) for q in quarter]
        core_far = [swap_core(q) for q in far_quarter]

        def columns(pieces, row):
            return [(g, 0, row, n) for n, g in enumerate(pieces)]

        groups = [
            [(half, 1, 0, 0), *columns(quarter, 0)],
            [(core_half, 1, 2, 0), *columns(core_quarter, 2)],
            [*columns(far_quarter, 1), *columns(core_far, 3)],
        ]
        steps = [adamw_steps(group) for group in groups]
        table = np.array(sum(steps, []), np.int32).T
        owns = jnp.where(table[0] == 0, 2 * core + chip, 2 * core).astype(jnp.int32)
        table = jnp.asarray(table) ^ (jnp.asarray([[0], [1], [0]], jnp.int32) * owns)
        out, begin = [], 0
        for n, group in enumerate(groups):
            out = adamw_blocks(group, table, begin, factor, arrays, out)
            begin += len(steps[n])
        return tuple(out)

    return jax.shard_map(
        step,
        mesh=mesh,
        in_specs=(P(("rep", "dp"), None, None),) * 2 + (P(None, None, None),) * 9,
        out_specs=(P("rep", None, None),) * 9,
        check_vma=False,
    )
```
